32 devices in a mesh: section: 8 (over z, core), head: 4 (over y, x).
Axes of the slice: x: 2, y: 2, z: 4, core: 2. Of those that a mesh axis runs over, the one named last changes fastest.
Arguments:
- out_grad: bfloat16 [2048, 8192], P('section', 'head'), may hold values from -6 to 6
- held_query: bfloat16 [2048, 8192], P('section', 'head'), may hold values from -90 to 90
- held_output: bfloat16 [2048, 8192], P('section', 'head'), may hold values from -6 to 6
- key_cache: bfloat16 [10240, 512], P(('section', 'head')), may hold values from -4 to 4
- value_cache: bfloat16 [10240, 512], P(('section', 'head')), may hold values from -6 to 6
- segment_ids: int32 [2048], P('section'), may hold values from 0 to 127, never falling along the last dimension, each value on 1 to 64 neighbouring positions
- image_flags: int32 [2048], P('section'), may hold values 0 or 1
- cache_length: int32 [8], P('section'), may hold values from 1024 to 2048, as said below
- query_weight: bfloat16 [16384, 8192], P('section', 'head'), may hold values from -0.09375 to 0.09375
- kv_weight: bfloat16 [16384, 1024], P('section', 'head'), may hold values from -0.09375 to 0.09375
- norm_gain: bfloat16 [16384], P('section'), may hold values from 0.5 to 1.5
- layer_input: bfloat16 [2048, 4096], P(('section', 'head')), may hold values from -6 to 6
- residual_grad: bfloat16 [2048, 4096], P(('section', 'head')), may hold values from -3 to 3
Outputs:
- input_grad: bfloat16 [2048, 4096], P(('section', 'head'))
The draws below stay inside these ranges and needn't reach their ends.
Inputs may be any that keep to these rules, and one draw needn't show every extreme that they name: `cache_length`: the two section indices 2 k and 2 k + 1 hold the same count; some section holds 2048.
All inputs are finite; a program needn't handle non-finite values. No bound on the sum of `image_flags` on one device may be relied on, other than what follows from the above.
Results may differ from the reference program's by a relative error of at most 0.0047.
Values may be sent and summed in bfloat16 or wider, within the bound.
No kernel may reach another device: no remote copies, remote signals or barrier semaphores. Data moves between devices by JAX's collectives and lax.ppermute only.
A program may use at most 128 MiB of HBM per device.

```python
import math
import jax
import jax.numpy as jnp
import numpy as np
from jax import lax

D = 4096
HQ = 64
KVH = 4
HD = 128
SL = 256
CTX = 2048
TOKENS = 2048
KEY_ROWS = 10240
WEIGHT_ROWS = 16384
N_SECTION = 8


def draw_key_cache(key, part):
    values_drawn = jnp.clip(jax.random.normal(jax.random.fold_in(key, 11), (KEY_ROWS, KVH * HD), jnp.float32), -4.0, 4.0)
    return values_drawn.astype(jnp.bfloat16)


def draw_held_query(key, part):
    values_drawn = jnp.clip(jax.random.normal(jax.random.fold_in(key, 13), (TOKENS, HQ * HD), jnp.float32), -4.0, 4.0)
    return values_drawn.astype(jnp.bfloat16)


def draw_cache_length(key, part):
    sections = N_SECTION // 2
    counts = jax.random.randint(jax.random.fold_in(key, 17), (sections,), CTX // 2, CTX + 1)
    where_full = jax.random.randint(jax.random.fold_in(key, 19), (), 0, sections)
    counts = jnp.where(jnp.arange(sections) == where_full, CTX, counts)
    return jnp.repeat(counts, 2).astype(jnp.int32)


def set_ends(entries, rng, smallest, top_value):
    index_at = [jax.random.randint(jax.random.fold_in(rng, axis), (), 0, length) for axis, length in enumerate(entries.shape)]
    main_axis = entries.shape.index(max(entries.shape))
    next_to = index_at[:main_axis] + [(index_at[main_axis] + 1) % entries.shape[main_axis]] + index_at[main_axis + 1:]
    return entries.at[tuple(index_at)].set(smallest).at[tuple(next_to)].set(top_value)


def level_of(key, dims, shards, smallest, high):
    gain, own = 1.0, jax.random.fold_in(key, 6)
    for dim, blocks in shards:
        heights = jnp.exp(jax.random.uniform(jax.random.fold_in(own, dim), (blocks,), jnp.float32, smallest / len(shards), high / len(shards)))
        gain = gain * jnp.repeat(heights, dims[dim] // blocks).reshape([-1 if axis == dim else 1 for axis in range(len(dims))])
    return gain


def split_up(number_of, total, most, lean):
    weights = [(1 << 20) // math.isqrt(rank ** lean) + 1 for rank in range(2, number_of + 1)]
    surplus, holding = total - most - (number_of - 1), [1] * (number_of - 1)
    while surplus > 0:
        movable = [i for i in range(number_of - 1) if holding[i] < most]
        whole, budget = sum([weights[i] for i in movable]), surplus
        for i in movable:
            more = min(most - holding[i], max(1, budget * weights[i] // whole), surplus)
            holding[i] = holding[i] + more
            surplus = surplus - more
    return np.array([most] + holding)


def uneven_parts(key, number_of, total, reach, lean):
    if number_of == 2:
        one = jax.random.randint(key, (), max(1, total - reach), min(reach, total - 1) + 1)
        return jnp.stack([one, total - one])
    sizes = jnp.asarray(split_up(number_of, total, reach, lean), jnp.int32)
    pairs = (number_of - 1) // 2
    donor, taker = sizes[1:1 + 2 * pairs:2], sizes[2:2 + 2 * pairs:2]
    room = jnp.minimum(donor - 1, reach - taker)
    shifted = jax.random.randint(jax.random.fold_in(key, 1), (pairs,), 0, 1 << 20) % (room + 1)
    sizes = sizes.at[1:1 + 2 * pairs:2].set(donor - shifted).at[2:2 + 2 * pairs:2].set(taker + shifted)
    return sizes[jax.random.permutation(jax.random.fold_in(key, 2), number_of)]


def centred(own_key, dims, deviation, limit, cuts=(), kind=jnp.bfloat16):
    values = deviation * jax.random.normal(own_key, dims, jnp.float32)
    if cuts:
        values = values * level_of(own_key, dims, cuts, -0.22, 0.18)
    return jnp.clip(values, -limit, limit).astype(kind)


def setup_inputs(seed: int = 0) -> dict:
    key_of = jax.random.split(jax.random.key(seed), 14)
    return {
        "out_grad": centred(key_of[0], (TOKENS, HQ * HD), 1.0, 6.0, ((0, 8), (1, 4))),
        "held_query": draw_held_query(jax.random.fold_in(key_of[13], 71), 0),
        "held_output": centred(key_of[2], (TOKENS, HQ * HD), 1.0, 6.0, ((0, 8), (1, 4))),
        "key_cache": draw_key_cache(jax.random.fold_in(key_of[13], 71), 0),
        "value_cache": centred(key_of[4], (KEY_ROWS, KVH * HD), 1.0, 6.0, ((0, 32),)),
        "segment_ids": jnp.searchsorted(jnp.cumsum(uneven_parts(key_of[5], TOKENS // 16, TOKENS, 64, 0)), jnp.arange(TOKENS), side="right").astype(jnp.int32),
        "image_flags": set_ends((jax.random.randint(key_of[6], (TOKENS,), 0, 2) < 1).astype(jnp.int32), jax.random.fold_in(key_of[6], 1), 0, 1),
        "cache_length": draw_cache_length(jax.random.fold_in(key_of[13], 71), 0),
        "query_weight": centred(key_of[8], (WEIGHT_ROWS, HQ * HD), D ** -0.5, 0.09375, ((0, 8), (1, 4))),
        "kv_weight": centred(key_of[9], (WEIGHT_ROWS, 2 * KVH * HD), D ** -0.5, 0.09375, ((0, 8), (1, 4))),
        "norm_gain": jnp.clip(1.0 + 0.1 * jax.random.normal(key_of[10], (WEIGHT_ROWS,), jnp.float32), 0.5, 1.5).astype(jnp.bfloat16),
        "layer_input": centred(key_of[11], (TOKENS, D), 1.0, 6.0, ((0, 32),)),
        "residual_grad": centred(key_of[12], (TOKENS, D), 0.5, 3.0, ((0, 32),)),
    }


epsilon = 1e-06
far_negative = -1e+30

def section_backward(operands):
    queries, outputs, grads, key_section, value_section, segment, image_mask, length, q_weight, kvw_section, gain_row, inputs, residual = operands
    group_size = HQ // KVH
    factor = 1.0 / math.sqrt(HD)
    row_total = 2 * SL
    positions = jnp.arange(row_total, dtype=jnp.int32)
    cache_ok = jnp.arange(CTX, dtype=jnp.int32)[None, :] < length
    cache_ok = jnp.broadcast_to(cache_ok, (row_total, CTX))
    same_segment = segment[:, None] == segment[None, :]
    both_image = (image_mask[:, None] == 1) & (image_mask[None, :] == 1)
    slice_ok = same_segment & ((positions[None, :] <= positions[:, None]) | both_image)
    visible = jnp.concatenate([cache_ok, slice_ok], axis=1)
    query_parts = []
    key_parts = []
    value_parts = []
    for head_group in range(KVH):
        lower = head_group * group_size * HD
        upper = (head_group + 1) * group_size * HD
        query_heads = queries[:, lower:upper].reshape(row_total, group_size, HD).astype(jnp.float32)
        output_heads = outputs[:, lower:upper].reshape(row_total, group_size, HD).astype(jnp.float32)
        grad_heads = grads[:, lower:upper].reshape(row_total, group_size, HD).astype(jnp.float32)
        key_part = key_section[:, head_group * HD:(head_group + 1) * HD].astype(jnp.float32)
        value_part = value_section[:, head_group * HD:(head_group + 1) * HD].astype(jnp.float32)
        scores = jnp.einsum('agd,jd->gaj', query_heads, key_part) * factor
        scores = jnp.where(visible[None], scores, far_negative)
        row_max = lax.optimization_barrier(jnp.max(scores, axis=2, keepdims=True))
        log_total = row_max + jnp.log(lax.optimization_barrier(jnp.sum(jnp.exp(scores - row_max), axis=2, keepdims=True)))
        attn_probs = jnp.exp(scores - log_total)
        probs_rounded = attn_probs.astype(jnp.bfloat16)
        prob_grad = jnp.einsum('agd,jd->gaj', grad_heads, value_part)
        row_delta = jnp.einsum('agd,agd->ga', grad_heads, output_heads)[..., None]
        score_grad = (attn_probs * (prob_grad - row_delta) * factor).astype(jnp.bfloat16)
        query_grad = jnp.einsum('gaj,jd->agd', score_grad.astype(jnp.float32), key_part)
        query_parts.append(query_grad.astype(jnp.bfloat16).reshape(row_total, group_size * HD))
        key_parts.append(jnp.einsum('gab,agd->bd', score_grad[..., CTX:].astype(jnp.float32), query_heads))
        value_parts.append(jnp.einsum('gab,agd->bd', probs_rounded[..., CTX:].astype(jnp.float32), grad_heads))
    query_all = jnp.concatenate(query_parts, axis=1)
    kv_grad = jnp.concatenate(key_parts + value_parts, axis=1)
    kv_rounded = kv_grad.astype(jnp.bfloat16)
    normed_grad = jnp.dot(query_all, q_weight.T, preferred_element_type=jnp.float32)
    normed_grad = normed_grad + jnp.dot(kv_rounded, kvw_section.T, preferred_element_type=jnp.float32)
    values_in = inputs.astype(jnp.float32)
    inverse = lax.rsqrt(lax.optimization_barrier(jnp.mean(values_in * values_in, axis=1, keepdims=True)) + epsilon)
    weighted = gain_row.astype(jnp.float32)[None, :] * normed_grad
    result = residual.astype(jnp.float32) + inverse * weighted - values_in * inverse ** 3 * lax.optimization_barrier(jnp.mean(weighted * values_in, axis=1, keepdims=True))
    return result.astype(jnp.bfloat16)

def reference(out_grad, held_query, held_output, key_cache, value_cache, segment_ids, image_flags, cache_length, query_weight, kv_weight, norm_gain, layer_input, residual_grad):
    sections = N_SECTION // 2
    queries = held_query.reshape(sections, 2 * SL, HQ * HD)[::-1]
    outputs = held_output.reshape(sections, 2 * SL, HQ * HD)[::-1]
    grads = out_grad.reshape(sections, 2 * SL, HQ * HD)
    key_section = key_cache.reshape(sections, CTX + 2 * SL, KVH * HD)
    value_section = value_cache.reshape(sections, CTX + 2 * SL, KVH * HD)
    segment = segment_ids.reshape(sections, 2 * SL)
    image_mask = image_flags.reshape(sections, 2 * SL)
    lengths = cache_length.reshape(sections, 2)[:, 0]
    q_weight = query_weight.reshape(sections, D, HQ * HD)
    kvw_section = kv_weight.reshape(sections, D, 2 * KVH * HD)
    gain_row = norm_gain.reshape(sections, D)
    inputs = layer_input.reshape(sections, 2 * SL, D)
    residual = residual_grad.reshape(sections, 2 * SL, D)
    result = lax.map(section_backward, (queries, outputs, grads, key_section, value_section, segment, image_mask, lengths, q_weight, kvw_section, gain_row, inputs, residual))
    return result.reshape(N_SECTION * SL, D)
```

```python
import functools
import math

import jax
import jax.numpy as jnp
from jax import lax
from jax.experimental import pallas as pl
from jax.experimental.pallas import tpu as pltpu
from jax.sharding import PartitionSpec as P


KVH = 4
HD = 128
SL = 256
CTX = 2048

epsilon = 1e-06
far_negative = -1e30
factor = 1.0 / math.sqrt(HD)
log2_factor = factor * math.log2(math.e)

CHUNK_EIGHTHS = (4, 2, 2)
ROW_BLOCK = 512
KEY_BLOCK = 512
FEATURE_TILE = 512


NT = (((1,), (1,)), ((), ()))
TN = (((0,), (0,)), ((), ()))
NN = (((1,), (0,)), ((), ()))


def dot(left, right, dims):
    return lax.dot_general(left, right, dims, preferred_element_type=jnp.float32)


def xor_pairs(axis, mask):
    return [(i, i ^ mask) for i in range(lax.axis_size(axis))]


def inward_pairs(section_count):
    if section_count != 8:
        return []
    return [(0, 2), (1, 3), (6, 4), (7, 5)]


def chunk_plan(group_tokens):
    if group_tokens % 64:
        half = group_tokens // 2
        return [(0, half), (half, group_tokens - half)]
    plan, start = [], 0
    for eighths in CHUNK_EIGHTHS:
        count = group_tokens * eighths // 8
        plan.append((start, count))
        start += count
    return plan


def lane_tiles(values):
    return [values[:, j * HD:(j + 1) * HD] for j in range(values.shape[1] // HD)]


def fold(op, tiles):
    out = tiles[0]
    for tile in tiles[1:]:
        out = op(out, tile)
    return out


def attention_kernel(
    scal_ref, *refs, tokens, local_heads, head_count, paired,
):
    if paired:
        q_ref, o_ref, refs = refs[0].at[0], refs[0].at[1], refs[1:]
    else:
        q_ref, o_ref, refs = refs[0], refs[1], refs[2:]
    g_ref, cache_ref, slice_ref, bias_c_ref, bias_s_ref, prev_own_ref, prev_next_ref = refs[:7]
    own_ref, other_ref, kv_own_ref, kv_next_ref = refs[7:11]
    outs = refs[11:11 + head_count]
    s_ref, dq_ref, weights, groups, sems = refs[11 + head_count:]
    kc_ref, vc_ref = cache_ref.at[0], cache_ref.at[1]
    ks_ref, vs_ref = slice_ref.at[0], slice_ref.at[1]
    parity, head = scal_ref[0], scal_ref[1]
    heads = min(local_heads, max(1, ROW_BLOCK // tokens))
    blocks = local_heads // heads
    cache_blocks = CTX // KEY_BLOCK
    half, tile = weights.shape[1], groups.shape[2]
    tiles = half // tile
    count = tokens // head_count

    def weight_copy(side, index):
        rows = pl.ds(index * tile, tile)
        source = own_ref if side == 0 else other_ref
        return pltpu.make_async_copy(
            source.at[rows], weights.at[side, rows], sems.at[side * tiles + index]
        )

    for side in range(2):
        for index in range(tiles):
            weight_copy(side, index).start()
    kv_own_ref[...] = prev_own_ref[...]
    kv_next_ref[...] = prev_next_ref[...]

    def block(index, carry):
        def rows_of(ref):
            parts = [
                ref[..., pl.ds(pl.multiple_of((index * heads + j) * HD, HD), HD)].reshape(tokens, HD)
                for j in range(heads)
            ]
            return parts[0] if heads == 1 else jnp.concatenate(parts, axis=0)

        q_rows, g_rows = rows_of(q_ref), rows_of(g_ref)
        delta = jnp.sum(
            g_rows.astype(jnp.float32) * rows_of(o_ref).astype(jnp.float32), axis=1, keepdims=True
        )
        running = None
        for kb in range(cache_blocks):
            keys = slice(kb * KEY_BLOCK, (kb + 1) * KEY_BLOCK)
            scores = dot(q_rows, kc_ref[keys, :], NT)
            if (kb + 1) * KEY_BLOCK > CTX // 2:
                scores = scores + bias_c_ref[:, keys]
            s_ref[:, keys] = scores
            top = fold(jnp.maximum, lane_tiles(scores))
            running = top if running is None else jnp.maximum(running, top)
        bias = bias_s_ref[...].reshape(tokens, bias_s_ref.shape[-1])
        scores = dot(q_rows, ks_ref[...], NT) + (
            bias if heads == 1 else jnp.concatenate([bias] * heads, axis=0)
        )
        s_ref[:, CTX:] = scores
        running = jnp.maximum(running, fold(jnp.maximum, lane_tiles(scores)))
        shift = jnp.max(running, axis=1, keepdims=True) * log2_factor

        total = None
        query_grad = None
        for kb in range(cache_blocks):
            keys = slice(kb * KEY_BLOCK, (kb + 1) * KEY_BLOCK)
            probs = jnp.exp2(s_ref[:, keys] * log2_factor - shift)
            part = fold(jnp.add, lane_tiles(probs))
            total = part if total is None else total + part
            prob_grad = dot(g_rows, vc_ref[keys, :], NT)
            score_grad = (probs * (prob_grad - delta)).astype(jnp.bfloat16)
            term = dot(score_grad, kc_ref[keys, :], NN)
            query_grad = term if query_grad is None else query_grad + term
        probs = jnp.exp2(s_ref[:, CTX:] * log2_factor - shift)
        total = total + fold(jnp.add, lane_tiles(probs))
        scale = 1.0 / jnp.sum(total, axis=1, keepdims=True)
        probs = probs * scale
        prob_grad = dot(g_rows, vs_ref[...], NT)
        score_grad = (probs * (prob_grad - delta) * factor).astype(jnp.bfloat16)
        query_grad = query_grad * (scale * factor) + dot(score_grad, ks_ref[...], NN)
        key_grad = dot(q_rows, score_grad, TN)
        value_grad = dot(g_rows, probs.astype(jnp.bfloat16), TN)
        for ref, keys in ((kv_own_ref, slice(0, SL)), (kv_next_ref, slice(SL, 2 * SL))):
            ref[:HD, :] += key_grad[:, keys]
            ref[HD:, :] += value_grad[:, keys]
        query_grad = query_grad.astype(jnp.bfloat16)
        for j in range(heads):
            dq_ref[:, pl.ds(pl.multiple_of((index * heads + j) * HD, HD), HD)] = query_grad[
                j * tokens:(j + 1) * tokens
            ]
        return carry

    lax.fori_loop(0, blocks, block, 0)

    for side in range(2):

        def project(index, carry):
            weight_copy(side, index).wait()
            rows = pl.ds(pl.multiple_of(index * tile, tile), tile)
            result = dot(dq_ref[...], weights[side, rows, :], NT)
            for group in range(head_count):
                groups[group] = result[group * count:(group + 1) * count]
            place = parity if side == 0 else 1 - parity
            lanes = pl.ds(pl.multiple_of(place * half + index * tile, tile), tile)
            for d, out in enumerate(outs):
                out[:, lanes] = groups[head ^ d].astype(jnp.bfloat16)
            return carry

        lax.fori_loop(0, tiles, project, 0)


def whole_block(array):
    return pl.BlockSpec(array.shape, lambda step: (0,) * array.ndim)


def token_block(array, start, count, head_count):
    width = array.shape[1]
    grouped = array.reshape(head_count, array.shape[0] // head_count, width)
    if start % count == 0 and count % 16 == 0:
        return grouped, pl.BlockSpec((head_count, count, width), lambda step: (0, start // count, 0))
    rows = grouped[:, start:start + count].reshape(head_count * count, width)
    return rows, whole_block(rows)


def attention(scal, stash, grads, cache, current, bias_c, biases, prev, own, other, head_count):
    tokens, width = stash[0].shape[-2:]
    local_heads = width // HD
    heads = min(local_heads, max(1, ROW_BLOCK // tokens))
    keys = cache.shape[1] + current.shape[1]
    half = own.shape[0]
    tile = min(half, FEATURE_TILE)
    count = tokens // head_count
    operands = [(array, whole_block(array)) for array in stash]
    operands += [grads] + [(array, whole_block(array)) for array in (cache, current, bias_c)]
    operands += [biases] + [(array, whole_block(array)) for array in prev]
    operands += [(array, pl.BlockSpec(memory_space=pl.ANY)) for array in (own, other)]
    results = [jax.ShapeDtypeStruct(array.shape, jnp.float32) for array in prev]
    results += [jax.ShapeDtypeStruct((count, 2 * half), jnp.bfloat16) for _ in range(head_count)]
    outs = pl.pallas_call(
        functools.partial(
            attention_kernel,
            tokens=tokens,
            local_heads=local_heads,
            head_count=head_count,
            paired=len(stash) == 1,
        ),
        out_shape=results,
        grid=(1,),
        in_specs=[pl.BlockSpec(memory_space=pltpu.SMEM)] + [spec for _, spec in operands],
        out_specs=[whole_block(result) for result in results],
        scratch_shapes=[
            pltpu.VMEM((heads * tokens, keys), jnp.float32),
            pltpu.VMEM((tokens, width), jnp.bfloat16),
            pltpu.VMEM((2, half, width), jnp.bfloat16),
            pltpu.VMEM((head_count, count, tile), jnp.float32),
            pltpu.SemaphoreType.DMA((2 * (half // tile),)),
        ],
        compiler_params=pltpu.CompilerParams(vmem_limit_bytes=48 * 2**20),
        cost_estimate=pl.CostEstimate(
            flops=24 * tokens * local_heads * keys * HD,
            bytes_accessed=4 * tokens * width * 2 + keys * HD * 4 + 4 * half * width,
            transcendentals=tokens * local_heads * keys,
        ),
        name="attention",
    )(scal, *[array for array, _ in operands])
    return outs[:2], outs[2:]


def pack_kernel(q_ref, o_ref, *outs, plan, group_tokens, head_count):
    for out, (start, count) in zip(outs, plan):
        for group in range(head_count):
            rows = slice(group * group_tokens + start, group * group_tokens + start + count)
            out[0, group * count:(group + 1) * count] = q_ref[rows]
            out[1, group * count:(group + 1) * count] = o_ref[rows]


def pack(q, o, plan, group_tokens, head_count):
    tokens, width = q.shape
    lanes = min(width, 512)
    return pl.pallas_call(
        functools.partial(
            pack_kernel, plan=plan, group_tokens=group_tokens, head_count=head_count
        ),
        out_shape=[
            jax.ShapeDtypeStruct((2, head_count * count, width), q.dtype) for _, count in plan
        ],
        grid=(width // lanes,),
        in_specs=[pl.BlockSpec((tokens, lanes), lambda step: (0, step))] * 2,
        out_specs=[
            pl.BlockSpec((2, head_count * count, lanes), lambda step: (0, 0, step))
            for _, count in plan
        ],
        name="pack",
    )(q, o)


def share_kernel(scal_ref, own_ref, recv_ref, *outs):
    head = scal_ref[1]
    count = outs[0].shape[0]
    total = (own_ref[...] + recv_ref[...]).T
    head_count = len(outs)
    for d, out in enumerate(outs):
        for group in range(head_count):

            @pl.when((head ^ d) == group)
            def _():
                out[...] = total[group * count:(group + 1) * count].astype(out.dtype)


def share_kv(scal, own, recv, head_count, dtype):
    width, tokens = own.shape
    count = tokens // head_count
    results = [jax.ShapeDtypeStruct((count, width), dtype) for _ in range(head_count)]
    return pl.pallas_call(
        share_kernel,
        out_shape=results,
        grid=(1,),
        in_specs=[pl.BlockSpec(memory_space=pltpu.SMEM), whole_block(own), whole_block(recv)],
        out_specs=[whole_block(result) for result in results],
        cost_estimate=pl.CostEstimate(
            flops=tokens * width, bytes_accessed=tokens * width * 10, transcendentals=0
        ),
        name="share",
    )(scal, own, recv)


def finish_kernel(
    scal_ref, gain_ref, x_ref, res_ref, *refs, plan, head_count, shares, spent, columns
):
    kv_pieces, refs = refs[:head_count], refs[head_count:]
    pieces, refs = refs[:shares], refs[shares + spent:]
    sources, refs = refs[:2 * columns], refs[2 * columns:]
    out_ref, gathered, total_ref, weights, sems = refs
    parity, head = scal_ref[0], scal_ref[1]
    sharers = head_count // KVH
    half, width = sources[0].shape

    def weight_copy(index):
        return pltpu.make_async_copy(sources[index], weights.at[index], sems.at[index])

    for index in range(2 * columns):
        weight_copy(index).start()
    if sharers > 1:
        gathered[...] = jnp.zeros_like(gathered)
    for d, piece in enumerate(kv_pieces):
        group = (head ^ d) // sharers
        for part in range(2):
            lanes = pl.ds(pl.multiple_of(group * HD + part * KVH * HD, HD), HD)
            value = piece[:, part * HD:(part + 1) * HD].astype(jnp.float32)
            if sharers > 1:
                value = gathered[:, lanes] + value
            gathered[:, lanes] = value
    for c, (start, count) in enumerate(plan):
        rows = slice(start, start + count)
        total_ref[rows, :] = fold(
            jnp.add,
            [pieces[c * head_count + d][...].astype(jnp.float32) for d in range(head_count)],
        )
    x = x_ref[...].astype(jnp.float32)
    inverse = lax.rsqrt(jnp.mean(x * x, axis=1, keepdims=True) + epsilon)
    for index in range(2 * columns):
        side, column = index // columns, index % columns
        if columns == 1:
            left = gathered[...]
        else:
            left = gathered[:, pl.ds(pl.multiple_of((head ^ column) * width, width), width)]
        left = left.astype(jnp.bfloat16)
        place = parity if side == 0 else 1 - parity
        lanes = pl.ds(pl.multiple_of(place * half, half), half)
        weight_copy(index).wait()
        total_ref[:, lanes] += dot(left, weights[index], NT)
    weighted = gain_ref[...].astype(jnp.float32) * total_ref[...]
    mean = jnp.mean(weighted * x, axis=1, keepdims=True)
    out_ref[...] = (
        res_ref[...].astype(jnp.float32)
        + inverse * weighted
        - x * (inverse * inverse * inverse * mean)
    ).astype(out_ref.dtype)


def finish(scal, gain, x, residual, kv_pieces, pieces, spent, weights, plan):
    head_count = len(kv_pieces)
    half, width = weights[0].shape
    columns = len(weights) // 2
    rows = x.shape[0]
    local = [gain, x, residual, *kv_pieces, *pieces]
    remote = [*spent, *weights]
    return pl.pallas_call(
        functools.partial(
            finish_kernel,
            plan=plan,
            head_count=head_count,
            shares=len(pieces),
            spent=len(spent),
            columns=columns,
        ),
        out_shape=jax.ShapeDtypeStruct(x.shape, jnp.bfloat16),
        grid=(1,),
        in_specs=[pl.BlockSpec(memory_space=pltpu.SMEM)]
        + [whole_block(array) for array in local]
        + [pl.BlockSpec(memory_space=pl.ANY) for _ in remote],
        out_specs=whole_block(x),
        scratch_shapes=[
            pltpu.VMEM((rows, 2 * KVH * HD), jnp.float32),
            pltpu.VMEM((rows, 2 * half), jnp.float32),
            pltpu.VMEM((2 * columns, half, width), jnp.bfloat16),
            pltpu.SemaphoreType.DMA((2 * columns,)),
        ],
        compiler_params=pltpu.CompilerParams(vmem_limit_bytes=40 * 2**20),
        cost_estimate=pl.CostEstimate(
            flops=512 * half * width * columns,
            bytes_accessed=4 * half * width * columns,
            transcendentals=0,
        ),
        name="finish",
    )(scal, *local, *remote)


def body(
    out_grad,
    held_query,
    held_output,
    key_cache,
    value_cache,
    segment_ids,
    image_flags,
    cache_length,
    query_weight,
    kv_weight,
    norm_gain,
    layer_input,
    residual_grad,
):
    head_count = lax.axis_size("head")
    section_count = lax.axis_size("section")
    head = lax.axis_index("head")
    parity = lax.axis_index("section") % 2
    is_first = parity == 0
    sharers = head_count // KVH
    group_tokens = SL // head_count
    plan = chunk_plan(group_tokens)
    scal = jnp.stack([parity, head]).astype(jnp.int32)

    def rows_of_chunk(array, start, count):
        grouped = array.reshape(head_count, group_tokens, array.shape[1])
        return grouped[:, start:start + count].reshape(head_count * count, array.shape[1])

    def swap_cores(value):
        return lax.ppermute(value, "section", xor_pairs("section", 1))

    def ordered(own_value, other_value, axis):
        return jnp.where(
            is_first,
            jnp.concatenate([own_value, other_value], axis),
            jnp.concatenate([other_value, own_value], axis),
        )

    mirror = xor_pairs("section", section_count - 2)
    inward = inward_pairs(section_count)
    first = [rows_of_chunk(held_query, *plan[0]), rows_of_chunk(held_output, *plan[0])]
    first, (held_query, held_output) = lax.optimization_barrier((first, (held_query, held_output)))
    buffers = pack(held_query, held_output, plan[1:], group_tokens, head_count)
    buffers, (key_cache, value_cache, kv_weight, query_weight) = lax.optimization_barrier(
        (buffers, (key_cache, value_cache, kv_weight, query_weight))
    )
    stash, spent = [], []
    for c, group in enumerate([first] + [[buffer] for buffer in buffers]):
        stash.append([])
        for buffer in group:
            stash[-1].append(lax.ppermute(buffer, "section", mirror))
        for buffer in group:
            if inward and c + 1 < len(plan):
                spent.append(lax.ppermute(buffer, "section", inward))

    pair_rows = jnp.stack([key_cache, value_cache])
    rows_here = pair_rows.shape[1]
    own_half = jnp.zeros((2, head_count * rows_here, HD), jnp.bfloat16)
    for d in range(head_count):
        target = head ^ d
        piece = lax.dynamic_slice_in_dim(pair_rows, target // sharers * HD, HD, 2)
        if d:
            piece = lax.ppermute(piece, "head", xor_pairs("head", d))
        own_half = lax.dynamic_update_slice_in_dim(own_half, piece, target * rows_here, 1)
    other_half, other_gain = swap_cores((own_half, norm_gain))
    both = ordered(own_half, other_half, 1)
    gain = ordered(norm_gain, other_gain, 0)[None, :]
    cache_rows = both[:, :CTX]
    own_rows = lax.dynamic_slice_in_dim(both, CTX + parity * SL, SL, 1)
    next_rows = lax.dynamic_slice_in_dim(both, CTX + (1 - parity) * SL, SL, 1)
    slice_rows = jnp.concatenate([own_rows, next_rows], 1)

    other_segments, other_flags = swap_cores((segment_ids, image_flags))
    positions = jnp.arange(SL, dtype=jnp.int32)
    own_position = parity * SL + positions
    key_position = jnp.concatenate([own_position, (1 - parity) * SL + positions])
    key_segments = jnp.concatenate([segment_ids, other_segments])
    key_flags = jnp.concatenate([image_flags, other_flags])
    visible = (segment_ids[:, None] == key_segments[None, :]) & (
        (key_position[None, :] <= own_position[:, None])
        | ((image_flags[:, None] == 1) & (key_flags[None, :] == 1))
    )
    bias_s = jnp.where(visible, 0.0, far_negative).astype(jnp.float32)
    bias_c = jnp.where(
        jnp.arange(CTX, dtype=jnp.int32)[None, :] < cache_length[0], 0.0, far_negative
    ).astype(jnp.float32)

    other_weight = swap_cores(query_weight)
    column_width = kv_weight.shape[1]
    kv_columns = [kv_weight]
    for d in range(1, head_count):
        kv_columns.append(lax.ppermute(kv_weight, "head", xor_pairs("head", d)))
    if column_width % HD:
        kv_rows = jnp.zeros((kv_weight.shape[0], head_count * column_width), jnp.bfloat16)
        for d, piece in enumerate(kv_columns):
            kv_rows = lax.dynamic_update_slice_in_dim(kv_rows, piece, (head ^ d) * column_width, 1)
        kv_columns = [kv_rows]
    for d in range(len(kv_columns)):
        kv_columns.append(swap_cores(kv_columns[d]))

    kv_grad = [jnp.zeros((2 * HD, SL), jnp.float32)] * 2
    pieces = []
    for c, (start, count) in enumerate(plan):
        kv_grad, parts = attention(
            scal,
            stash[c],
            token_block(out_grad, start, count, head_count),
            cache_rows,
            slice_rows,
            bias_c,
            token_block(bias_s, start, count, head_count),
            kv_grad,
            query_weight,
            other_weight,
            head_count,
        )
        for d, part in enumerate(parts):
            pieces.append(lax.ppermute(part, "head", xor_pairs("head", d)) if d else part)
    received = swap_cores(kv_grad[1])
    share_dtype = jnp.bfloat16 if sharers == 1 else jnp.float32
    shares = list(share_kv(scal, kv_grad[0], received, head_count, share_dtype))
    for d in range(1, head_count):
        shares[d] = lax.ppermute(shares[d], "head", xor_pairs("head", d))
    return finish(
        scal, gain, layer_input, residual_grad, shares, pieces, spent, kv_columns, plan
    )


def solution(mesh):
    return jax.shard_map(
        body,
        mesh=mesh,
        in_specs=(
            P("section", "head"),
            P("section", "head"),
            P("section", "head"),
            P(("section", "head"), None),
            P(("section", "head"), None),
            P("section"),
            P("section"),
            P("section"),
            P("section", "head"),
            P("section", "head"),
            P("section"),
            P(("section", "head"), None),
            P(("section", "head"), None),
        ),
        out_specs=P(("section", "head"), None),
        check_vma=False,
    )
```

```python
import functools
import math

import jax
import jax.numpy as jnp
from jax import lax
from jax.experimental import pallas as pl
from jax.experimental.pallas import tpu as pltpu
from jax.sharding import PartitionSpec as P


KVH = 4
HD = 128
SL = 256
CTX = 2048
REACH = 128

epsilon = 1e-06
far_negative = -1e30
factor = 1.0 / math.sqrt(HD)
log2_factor = factor * math.log2(math.e)

CHUNK_EIGHTHS = (4, 2, 2)
ROW_BLOCK = 512
KEY_BLOCK = 512
FEATURE_TILE = 1024
VMEM_LIMIT = 46 * 2**20
LAST_VMEM_LIMIT = 46 * 2**20


NT = (((1,), (1,)), ((), ()))
TN = (((0,), (0,)), ((), ()))
NN = (((1,), (0,)), ((), ()))


def dot(left, right, dims):
    return lax.dot_general(left, right, dims, preferred_element_type=jnp.float32)


def xor_pairs(axis, mask):
    return [(i, i ^ mask) for i in range(lax.axis_size(axis))]


def inward_pairs(section_count):
    if section_count != 8:
        return []
    return [(0, 2), (1, 3), (6, 4), (7, 5)]


def chunk_plan(group_tokens):
    if group_tokens % 64:
        half = group_tokens // 2
        return [(0, half), (half, group_tokens - half)]
    plan, start = [], 0
    for eighths in CHUNK_EIGHTHS:
        count = group_tokens * eighths // 8
        plan.append((start, count))
        start += count
    return plan


def flush_points(plan):
    return {max(0, len(plan) - 2), len(plan) - 1}


def lane_tiles(values):
    return [values[:, j * HD:(j + 1) * HD] for j in range(values.shape[1] // HD)]


def fold(op, tiles):
    out = tiles[0]
    for tile in tiles[1:]:
        out = op(out, tile)
    return out


def attention_kernel(
    *refs, tokens, local_heads, head_count, paired, first, before, flush, grad_start
):
    if paired:
        q_ref, o_ref, refs = refs[0].at[0], refs[0].at[1], refs[1:]
    else:
        q_ref, o_ref, refs = refs[0], refs[1], refs[2:]
    g_ref, pair_ref, bias_c_ref, bias_s_ref, refs = *refs[:4], refs[4:]
    prev_refs, refs = ((), refs) if first else (refs[:2], refs[2:])
    dq_before, refs = refs[:len(before)], refs[len(before):]
    weight_refs, refs = (refs[:2], refs[2:]) if flush else ((), refs)
    kv_refs, refs = refs[:2], refs[2:]
    parity, head = lax.axis_index("section") % 2, lax.axis_index("head")
    heads = min(local_heads, max(1, ROW_BLOCK // tokens))
    blocks = local_heads // heads
    cache_blocks = CTX // KEY_BLOCK
    held = sum(before)
    if flush:
        outs, refs = refs[:head_count], refs[head_count:]
        s_ref, dq_ref, weights, groups, sems = refs
        half, tile = weights.shape[2], groups.shape[2]

        def weight_copy(side):
            return pltpu.make_async_copy(weight_refs[side], weights.at[side], sems.at[side])

        for side in range(2):
            weight_copy(side).start()
        row = 0
        for ref, rows in zip(dq_before, before):
            dq_ref[row:row + rows, :] = ref[...]
            row += rows
        dq_ref = dq_ref.at[held:]
    else:
        dq_ref, s_ref = refs
    for index, ref in enumerate(kv_refs):
        ref[...] = jnp.zeros_like(ref) if first else prev_refs[index][...]
    slice_parts = [
        (0, SL, pl.multiple_of(CTX + parity * SL, SL)),
        (SL, REACH, pl.multiple_of(CTX + SL - parity * REACH, REACH)),
    ]

    def block(index, carry):
        def rows_of(ref):
            parts = []
            for j in range(heads):
                lanes = pl.ds(pl.multiple_of((index * heads + j) * HD, HD), HD)
                part = ref[..., lanes]
                if part.size != tokens * HD:
                    part = part.astype(jnp.float32)[:, grad_start:grad_start + tokens // head_count]
                parts.append(part.reshape(tokens, HD).astype(jnp.bfloat16))
            return parts[0] if heads == 1 else jnp.concatenate(parts, axis=0)

        q_rows, g_rows = rows_of(q_ref), rows_of(g_ref)
        delta = jnp.sum(
            g_rows.astype(jnp.float32) * rows_of(o_ref).astype(jnp.float32), axis=1, keepdims=True
        )
        running = None
        for kb in range(cache_blocks):
            keys = slice(kb * KEY_BLOCK, (kb + 1) * KEY_BLOCK)
            scores = dot(q_rows, pair_ref[0, keys, :], NT)
            if (kb + 1) * KEY_BLOCK > CTX // 2:
                scores = scores + bias_c_ref[:, keys]
            s_ref[:, keys] = scores
            top = fold(jnp.maximum, lane_tiles(scores))
            running = top if running is None else jnp.maximum(running, top)
        bias = bias_s_ref[...].reshape(tokens, bias_s_ref.shape[-1])
        bias = bias if heads == 1 else jnp.concatenate([bias] * heads, axis=0)
        for lane, count, row in slice_parts:
            scores = dot(q_rows, pair_ref[0, pl.ds(row, count), :], NT) + bias[:, lane:lane + count]
            s_ref[:, CTX + lane:CTX + lane + count] = scores
            running = jnp.maximum(running, fold(jnp.maximum, lane_tiles(scores)))
        shift = jnp.max(running, axis=1, keepdims=True) * log2_factor

        total = None
        query_grad = None
        for kb in range(cache_blocks):
            keys = slice(kb * KEY_BLOCK, (kb + 1) * KEY_BLOCK)
            probs = jnp.exp2(s_ref[:, keys] * log2_factor - shift)
            part = fold(jnp.add, lane_tiles(probs))
            total = part if total is None else total + part
            prob_grad = dot(g_rows, pair_ref[1, keys, :], NT)
            score_grad = (probs * (prob_grad - delta)).astype(jnp.bfloat16)
            term = dot(score_grad, pair_ref[0, keys, :], NN)
            query_grad = term if query_grad is None else query_grad + term
        probs = jnp.exp2(s_ref[:, CTX:] * log2_factor - shift)
        total = total + fold(jnp.add, lane_tiles(probs))
        scale = 1.0 / jnp.sum(total, axis=1, keepdims=True)
        probs = probs * scale
        query_grad = query_grad * (scale * factor)
        for part, (lane, count, row) in enumerate(slice_parts):
            rows = pl.ds(row, count)
            part_probs = probs[:, lane:lane + count]
            prob_grad = dot(g_rows, pair_ref[1, rows, :], NT)
            score_grad = (part_probs * (prob_grad - delta) * factor).astype(jnp.bfloat16)
            query_grad = query_grad + dot(score_grad, pair_ref[0, rows, :], NN)
            kv_refs[part][:HD, :] += dot(q_rows, score_grad, TN)
            kv_refs[part][HD:, :] += dot(g_rows, part_probs.astype(jnp.bfloat16), TN)
        query_grad = query_grad.astype(jnp.bfloat16)
        for j in range(heads):
            dq_ref[:, pl.ds(pl.multiple_of((index * heads + j) * HD, HD), HD)] = query_grad[
                j * tokens:(j + 1) * tokens
            ]
        return carry

    lax.fori_loop(0, blocks, block, 0)
    if not flush:
        return

    all_rows = refs[1]
    spans, row, place = [], 0, 0
    for rows in (*before, tokens):
        spans.append((row, place, rows // head_count))
        row, place = row + rows, place + rows // head_count
    for side in range(2):
        weight_copy(side).wait()
        column = parity if side == 0 else 1 - parity

        def project(index, carry):
            source = pl.ds(pl.multiple_of(index * tile, tile), tile)
            result = dot(all_rows[...], weights[side, :, source], NN)
            for row, place, count in spans:
                for group in range(head_count):
                    start = row + group * count
                    groups[group, place:place + count] = result[start:start + count]
            lanes = pl.ds(pl.multiple_of(column * half + index * tile, tile), tile)
            for d, out in enumerate(outs):
                out[:, lanes] = groups[head ^ d].astype(jnp.bfloat16)
            return carry

        lax.fori_loop(0, half // tile, project, 0)


def whole_block(array):
    return pl.BlockSpec(array.shape, lambda step: (0,) * array.ndim)


def token_block(array, start, count, head_count, tile):
    width = array.shape[1]
    grouped = array.reshape(head_count, array.shape[0] // head_count, width)
    rows = max(count, tile)
    block = start // rows
    return (
        grouped,
        pl.BlockSpec((head_count, rows, width), lambda step: (0, block, 0)),
        start - block * rows,
    )


def attention(
    stash, grads, pair, bias_c, biases, prev, before, weights, head_count, vmem_limit
):
    tokens, width = stash[0].shape[-2:]
    local_heads = width // HD
    heads = min(local_heads, max(1, ROW_BLOCK // tokens))
    keys = CTX + SL + REACH
    flush = weights is not None
    operands = [(array, whole_block(array)) for array in stash]
    operands += [grads[:2]] + [(array, whole_block(array)) for array in (pair, bias_c)]
    operands += [biases[:2]]
    operands += [(array, whole_block(array)) for array in (*prev, *before)]
    results = [jax.ShapeDtypeStruct((2 * HD, count), jnp.float32) for count in (SL, REACH)]
    scratch = [pltpu.VMEM((heads * tokens, keys), jnp.float32)]
    cost = 3 * tokens * local_heads * keys * HD
    if flush:
        half = weights[0].shape[1]
        tile = min(half, FEATURE_TILE)
        rows = tokens + sum(array.shape[0] for array in before)
        count = rows // head_count
        operands += [(array, pl.BlockSpec(memory_space=pl.ANY)) for array in weights]
        results += [
            jax.ShapeDtypeStruct((count, 2 * half), jnp.bfloat16) for _ in range(head_count)
        ]
        scratch += [
            pltpu.VMEM((rows, width), jnp.bfloat16),
            pltpu.VMEM((2, width, half), jnp.bfloat16),
            pltpu.VMEM((head_count, count, tile), jnp.float32),
            pltpu.SemaphoreType.DMA((2,)),
        ]
        cost += 2 * rows * width * half
    else:
        results += [jax.ShapeDtypeStruct((tokens, width), jnp.bfloat16)]
    outs = pl.pallas_call(
        functools.partial(
            attention_kernel,
            tokens=tokens,
            local_heads=local_heads,
            head_count=head_count,
            paired=len(stash) == 1,
            first=not prev,
            before=tuple(array.shape[0] for array in before),
            flush=flush,
            grad_start=grads[2],
        ),
        out_shape=results,
        grid=(1,),
        in_specs=[spec for _, spec in operands],
        out_specs=[whole_block(result) for result in results],
        scratch_shapes=scratch,
        compiler_params=pltpu.CompilerParams(vmem_limit_bytes=vmem_limit),
        cost_estimate=pl.CostEstimate(
            flops=8 * cost,
            bytes_accessed=4 * tokens * width * 2 + keys * HD * 4,
            transcendentals=tokens * local_heads * keys,
        ),
        name="attention",
    )(*[array for array, _ in operands])
    return outs[:2], outs[2:]


def split_kernel(*refs, sharers):
    head = lax.axis_index("head")
    sources, outs = refs[:2], refs[2:]
    for d, out in enumerate(outs):
        lanes = pl.ds(pl.multiple_of((head ^ d) // sharers * HD, HD), HD)
        for index, source in enumerate(sources):
            out[index] = source[:, lanes]


def split_heads(arrays, head_count):
    rows = arrays[0].shape[0]
    results = [jax.ShapeDtypeStruct((2, rows, HD), arrays[0].dtype) for _ in range(head_count)]
    return pl.pallas_call(
        functools.partial(split_kernel, sharers=head_count // KVH),
        out_shape=results,
        grid=(1,),
        in_specs=[whole_block(array) for array in arrays],
        out_specs=[whole_block(result) for result in results],
        compiler_params=pltpu.CompilerParams(vmem_limit_bytes=VMEM_LIMIT),
        name="split",
    )(*arrays)


def arrange_kernel(*refs):
    pieces, out_ref = refs[:-1], refs[-1]
    parity, head = lax.axis_index("section") % 2, lax.axis_index("head")
    head_count = len(pieces) // 2
    rows = pieces[0].shape[1]
    for index, piece in enumerate(pieces):
        place = parity if index < head_count else 1 - parity
        start = (place * head_count + (head ^ index % head_count)) * rows
        out_ref[:, pl.ds(pl.multiple_of(start, 16), rows)] = piece[...]


def arrange(pieces):
    rows = pieces[0].shape[1]
    result = jax.ShapeDtypeStruct((2, len(pieces) * rows, HD), pieces[0].dtype)
    return pl.pallas_call(
        arrange_kernel,
        out_shape=result,
        grid=(1,),
        in_specs=[whole_block(piece) for piece in pieces],
        out_specs=whole_block(result),
        compiler_params=pltpu.CompilerParams(vmem_limit_bytes=VMEM_LIMIT),
        name="arrange",
    )(*pieces)


def pack_kernel(q_ref, o_ref, *outs, plan, group_tokens, head_count):
    for out, (start, count) in zip(outs, plan):
        for group in range(head_count):
            rows = slice(group * group_tokens + start, group * group_tokens + start + count)
            out[0, group * count:(group + 1) * count] = q_ref[rows]
            out[1, group * count:(group + 1) * count] = o_ref[rows]


def pack(q, o, plan, group_tokens, head_count):
    tokens, width = q.shape
    lanes = min(width, 512)
    return pl.pallas_call(
        functools.partial(
            pack_kernel, plan=plan, group_tokens=group_tokens, head_count=head_count
        ),
        out_shape=[
            jax.ShapeDtypeStruct((2, head_count * count, width), q.dtype) for _, count in plan
        ],
        grid=(width // lanes,),
        in_specs=[pl.BlockSpec((tokens, lanes), lambda step: (0, step))] * 2,
        out_specs=[
            pl.BlockSpec((2, head_count * count, lanes), lambda step: (0, 0, step))
            for _, count in plan
        ],
        name="pack",
    )(q, o)


def transpose_kernel(in_ref, out_ref):
    out_ref[...] = in_ref[...].T


def transposed(array):
    rows, columns = array.shape
    tile = math.gcd(rows, 512)
    return pl.pallas_call(
        transpose_kernel,
        out_shape=jax.ShapeDtypeStruct((columns, rows), array.dtype),
        grid=(rows // tile,),
        in_specs=[pl.BlockSpec((tile, columns), lambda step: (step, 0))],
        out_specs=pl.BlockSpec((columns, tile), lambda step: (0, step)),
        compiler_params=pltpu.CompilerParams(vmem_limit_bytes=VMEM_LIMIT),
        cost_estimate=pl.CostEstimate(
            flops=rows * columns, bytes_accessed=4 * rows * columns, transcendentals=0
        ),
        name="transposed",
    )(array)


def share_kernel(own_ref, recv_ref, *refs):
    outs, total_ref = refs[:-1], refs[-1]
    head = lax.axis_index("head")
    count = outs[0].shape[0]
    parity = lax.axis_index("section") % 2
    lanes = pl.ds(pl.multiple_of((1 - parity) * (SL - REACH), REACH), REACH)
    total_ref[...] = own_ref[...]
    total_ref[:, lanes] += recv_ref[...]
    total = total_ref[...].T
    head_count = len(outs)
    for d, out in enumerate(outs):
        for group in range(head_count):

            @pl.when((head ^ d) == group)
            def _():
                out[...] = total[group * count:(group + 1) * count].astype(out.dtype)


def share_kv(own, recv, head_count, dtype):
    width, tokens = own.shape
    count = tokens // head_count
    results = [jax.ShapeDtypeStruct((count, width), dtype) for _ in range(head_count)]
    return pl.pallas_call(
        share_kernel,
        out_shape=results,
        grid=(1,),
        in_specs=[whole_block(own), whole_block(recv)],
        out_specs=[whole_block(result) for result in results],
        scratch_shapes=[pltpu.VMEM(own.shape, jnp.float32)],
        compiler_params=pltpu.CompilerParams(vmem_limit_bytes=4*2**20),
        cost_estimate=pl.CostEstimate(
            flops=tokens * width, bytes_accessed=tokens * width * 10, transcendentals=0
        ),
        name="share",
    )(own, recv)


def finish_kernel(*refs, plan, head_count, spent):
    shares = len(plan) * head_count
    inputs = 3 + head_count + shares
    sources, refs = refs[:inputs], refs[inputs + spent:]
    weight_sources, refs = refs[:2 * head_count], refs[2 * head_count:]
    out_ref, refs = refs[0], refs[1:]
    locals_, refs = refs[:inputs], refs[inputs:]
    gathered, total_ref, input_sems = refs
    parity, head = lax.axis_index("section") % 2, lax.axis_index("head")
    sharers = head_count // KVH
    width, half = weight_sources[0].shape
    step = min(width, HD)

    def input_copy(index):
        return pltpu.make_async_copy(sources[index], locals_[index], input_sems.at[index])

    for index in range(inputs):
        input_copy(index).start()
    gain_ref, x_ref, res_ref = locals_[:3]
    kv_pieces, pieces = locals_[3:3 + head_count], locals_[3 + head_count:]
    for index in range(3, 3 + head_count):
        input_copy(index).wait()
    if sharers > 1:
        gathered[...] = jnp.zeros_like(gathered)
    for d, piece in enumerate(kv_pieces):
        group = (head ^ d) // sharers
        for part in range(2):
            column = group * HD + part * KVH * HD
            for lane in range(0, HD, step):
                place = (column + lane) // width
                lanes = pl.ds(pl.multiple_of((column + lane) % width, step), step)
                if step == width:
                    lanes = slice(0, width)
                value = piece[:, part * HD + lane:part * HD + lane + step].astype(jnp.float32)
                if sharers > 1:
                    value = gathered[place, :, lanes] + value
                gathered[place, :, lanes] = value
    for side in range(2):
        place = parity if side == 0 else 1 - parity
        lanes = pl.ds(pl.multiple_of(place * half, half), half)
        terms = []
        for d in range(head_count):
            left = gathered[head ^ d].astype(jnp.bfloat16)
            terms.append(dot(left, weight_sources[side * head_count + d][...], NN))
        total_ref[:, lanes] = fold(jnp.add, terms)
    for index in [*range(3), *range(3 + head_count, inputs)]:
        input_copy(index).wait()
    x = x_ref[...].astype(jnp.float32)
    inverse = lax.rsqrt(jnp.mean(x * x, axis=1, keepdims=True) + epsilon)
    for c, (start, count) in enumerate(plan):
        rows = slice(start, start + count)
        parts = [pieces[c * head_count + d][...].astype(jnp.float32) for d in range(head_count)]
        total = total_ref[rows, :] + fold(jnp.add, parts)
        total_ref[rows, :] = gain_ref[...].astype(jnp.float32) * total
    mean = jnp.mean(total_ref[...] * x_ref[...].astype(jnp.float32), axis=1, keepdims=True)
    mean = inverse * inverse * inverse * mean
    out_ref[...] = (
        res_ref[...].astype(jnp.float32)
        + inverse * total_ref[...]
        - x_ref[...].astype(jnp.float32) * mean
    ).astype(out_ref.dtype)


def finish(gain, x, residual, kv_pieces, pieces, spent, weights, plan):
    head_count = len(kv_pieces)
    width, half = weights[0].shape
    rows = x.shape[0]
    local = [gain, x, residual, *kv_pieces, *pieces]
    remote = [*spent, *weights]
    early = [pltpu.HBM] * (len(pieces) - head_count + 1)
    late = [pl.ANY] * (head_count - 1)
    spaces = [pltpu.HBM] * 3 + [pl.ANY] * head_count + early + late
    return pl.pallas_call(
        functools.partial(
            finish_kernel, plan=plan, head_count=head_count, spent=len(spent)
        ),
        out_shape=jax.ShapeDtypeStruct(x.shape, jnp.bfloat16),
        in_specs=[pl.BlockSpec(memory_space=space) for space in spaces]
        + [pl.BlockSpec(memory_space=pltpu.HBM) for _ in spent]
        + [pl.BlockSpec(memory_space=pltpu.VMEM) for _ in weights],
        out_specs=pl.BlockSpec(memory_space=pltpu.VMEM),
        scratch_shapes=[pltpu.VMEM(array.shape, array.dtype) for array in local]
        + [
            pltpu.VMEM((head_count, rows, width), jnp.float32),
            pltpu.VMEM((rows, 2 * half), jnp.float32),
            pltpu.SemaphoreType.DMA((len(local),)),
        ],
        compiler_params=pltpu.CompilerParams(vmem_limit_bytes=24*2**20),
        cost_estimate=pl.CostEstimate(
            flops=512 * half * width * head_count,
            bytes_accessed=4 * half * width * head_count,
            transcendentals=0,
        ),
        name="finish",
    )(*local, *remote)


def body(
    out_grad,
    held_query,
    held_output,
    key_cache,
    value_cache,
    segment_ids,
    image_flags,
    cache_length,
    query_weight,
    kv_weight,
    norm_gain,
    layer_input,
    residual_grad,
):
    head_count = lax.axis_size("head")
    section_count = lax.axis_size("section")
    parity = lax.axis_index("section") % 2
    is_first = parity == 0
    sharers = head_count // KVH
    group_tokens = SL // head_count
    plan = chunk_plan(group_tokens)

    def rows_of_chunk(array, start, count):
        grouped = array.reshape(head_count, group_tokens, array.shape[1])
        return grouped[:, start:start + count].reshape(head_count * count, array.shape[1])

    def swap_cores(value):
        return lax.ppermute(value, "section", xor_pairs("section", 1))

    def ordered(own_value, other_value, axis):
        return jnp.where(
            is_first,
            jnp.concatenate([own_value, other_value], axis),
            jnp.concatenate([other_value, own_value], axis),
        )

    mirror = xor_pairs("section", section_count - 2)
    inward = inward_pairs(section_count)
    first_query = rows_of_chunk(held_query, *plan[0])
    first_query, held_output = lax.optimization_barrier((first_query, held_output))
    first_output = rows_of_chunk(held_output, *plan[0])
    first = [first_query, first_output]
    first_output, held_query, held_output = lax.optimization_barrier(
        (first_output, held_query, held_output)
    )
    buffers = pack(held_query, held_output, plan[1:], group_tokens, head_count)
    buffers, (key_cache, value_cache, kv_weight, query_weight) = lax.optimization_barrier(
        (buffers, (key_cache, value_cache, kv_weight, query_weight))
    )
    stash, spent = [], []
    for c, group in enumerate([first] + [[buffer] for buffer in buffers]):
        stash.append([])
        for buffer in group:
            stash[-1].append(lax.ppermute(buffer, "section", mirror))
        if inward and c in (0, 1):
            spent.append(lax.ppermute(group[0] if c else held_query, "section", inward))

    other_segments = swap_cores(segment_ids)
    other_flags = swap_cores(image_flags)
    other_gain = swap_cores(norm_gain)
    gain = ordered(norm_gain, other_gain, 0)[None, :]

    split = split_heads((key_cache, value_cache), head_count)
    split, (query_weight, kv_weight) = lax.optimization_barrier((split, (query_weight, kv_weight)))
    key_pieces = [split[0]]
    for d in range(1, head_count):
        key_pieces.append(lax.ppermute(split[d], "head", xor_pairs("head", d)))
    for d in range(head_count):
        key_pieces.append(swap_cores(key_pieces[d]))
    pair = arrange(key_pieces)

    positions = jnp.arange(SL, dtype=jnp.int32)
    own_position = parity * SL + positions

    def with_reach(own_values, other_values):
        reach = lax.dynamic_slice_in_dim(other_values, parity * (SL - REACH), REACH)
        return jnp.concatenate([own_values, reach])

    key_position = with_reach(own_position, (1 - parity) * SL + positions)
    key_segments = with_reach(segment_ids, other_segments)
    key_flags = with_reach(image_flags, other_flags)
    visible = (segment_ids[:, None] == key_segments[None, :]) & (
        (key_position[None, :] <= own_position[:, None])
        | ((image_flags[:, None] == 1) & (key_flags[None, :] == 1))
    )
    bias_s = jnp.where(visible, 0.0, far_negative).astype(jnp.float32)
    bias_c = jnp.where(
        jnp.arange(CTX, dtype=jnp.int32)[None, :] < cache_length[0], 0.0, far_negative
    ).astype(jnp.float32)

    query_weight = transposed(query_weight)
    other_weight = swap_cores(query_weight)
    kv_columns = [kv_weight.T]
    for d in range(1, head_count):
        kv_columns.append(lax.ppermute(kv_columns[0], "head", xor_pairs("head", d)))
    for d in range(head_count):
        kv_columns.append(swap_cores(kv_columns[d]))
    gain, bias_c = lax.optimization_barrier((gain, bias_c))

    kv_grad, pieces, spans, before, first_row = (), [], [], [], 0
    flushes = flush_points(plan)
    for c, (start, count) in enumerate(plan):
        kv_grad, parts = attention(
            stash[c],
            token_block(out_grad, start, count, head_count, 16),
            pair,
            bias_c,
            token_block(bias_s, start, count, head_count, 8),
            kv_grad,
            before,
            (query_weight, other_weight) if c in flushes else None,
            head_count,
            VMEM_LIMIT if c + 1 < len(plan) else LAST_VMEM_LIMIT,
        )
        if c not in flushes:
            before = before + list(parts)
            continue
        for d, part in enumerate(parts):
            pieces.append(lax.ppermute(part, "head", xor_pairs("head", d)) if d else part)
        spans.append((first_row, start + count - first_row))
        first_row, before = start + count, []
    received = swap_cores(kv_grad[1])
    share_dtype = jnp.bfloat16 if sharers == 1 else jnp.float32
    shares = list(share_kv(kv_grad[0], received, head_count, share_dtype))
    for d in range(1, head_count):
        shares[d] = lax.ppermute(shares[d], "head", xor_pairs("head", d))
    return finish(
        gain, layer_input, residual_grad, shares, pieces, spent, kv_columns, spans
    )


def solution(mesh):
    return jax.shard_map(
        body,
        mesh=mesh,
        in_specs=(
            P("section", "head"),
            P("section", "head"),
            P("section", "head"),
            P(("section", "head"), None),
            P(("section", "head"), None),
            P("section"),
            P("section"),
            P("section"),
            P("section", "head"),
            P("section", "head"),
            P("section"),
            P(("section", "head"), None),
            P(("section", "head"), None),
        ),
        out_specs=P(("section", "head"), None),
        check_vma=False,
    )
```

```python
import functools
import math

import jax
import jax.numpy as jnp
from jax import lax
from jax.experimental import pallas as pl
from jax.experimental.pallas import tpu as pltpu
from jax.sharding import PartitionSpec as P


KVH = 4
HD = 128
SL = 256
CTX = 2048
REACH = 128

epsilon = 1e-06
far_negative = -1e30
factor = 1.0 / math.sqrt(HD)
log2_factor = factor * math.log2(math.e)

CHUNK_EIGHTHS = (4, 2, 2)
ROW_BLOCK = 1024
KEY_BLOCK = 512
FEATURE_TILE = 1024
VMEM_LIMIT = 46 * 2**20
LAST_VMEM_LIMIT = 46 * 2**20


NT = (((1,), (1,)), ((), ()))
TN = (((0,), (0,)), ((), ()))
NN = (((1,), (0,)), ((), ()))


def dot(left, right, dims):
    return lax.dot_general(left, right, dims, preferred_element_type=jnp.float32)


def xor_pairs(axis, mask):
    return [(i, i ^ mask) for i in range(lax.axis_size(axis))]


def inward_pairs(section_count):
    if section_count != 8:
        return []
    return [(0, 2), (1, 3), (6, 4), (7, 5)]


def chunk_plan(group_tokens):
    if group_tokens % 64:
        half = group_tokens // 2
        return [(0, half), (half, group_tokens - half)]
    plan, start = [], 0
    for eighths in CHUNK_EIGHTHS:
        count = group_tokens * eighths // 8
        plan.append((start, count))
        start += count
    return plan


def flush_points(plan):
    return {max(0, len(plan) - 2), len(plan) - 1}


def lane_tiles(values):
    return [values[:, j * HD:(j + 1) * HD] for j in range(values.shape[1] // HD)]


def fold(op, tiles):
    out = tiles[0]
    for tile in tiles[1:]:
        out = op(out, tile)
    return out


def attention_kernel(
    *refs, tokens, local_heads, head_count, paired, first, before, flush, grad_start
):
    if paired:
        q_ref, o_ref, refs = refs[0].at[0], refs[0].at[1], refs[1:]
    else:
        q_ref, o_ref, refs = refs[0], refs[1], refs[2:]
    g_ref, pair_ref, bias_c_ref, bias_s_ref, refs = *refs[:4], refs[4:]
    prev_refs, refs = ((), refs) if first else (refs[:2], refs[2:])
    dq_before, refs = refs[:len(before)], refs[len(before):]
    weight_refs, refs = (refs[:2], refs[2:]) if flush else ((), refs)
    kv_refs, refs = refs[:2], refs[2:]
    parity, head = lax.axis_index("section") % 2, lax.axis_index("head")
    heads = min(local_heads, max(1, ROW_BLOCK // tokens))
    blocks = local_heads // heads
    cache_blocks = CTX // KEY_BLOCK
    held = sum(before)
    if flush:
        outs, refs = refs[:head_count], refs[head_count:]
        s_ref, dq_ref, weights, groups, sems = refs
        half, tile = weights.shape[2], groups.shape[2]

        def weight_copy(side):
            return pltpu.make_async_copy(weight_refs[side], weights.at[side], sems.at[side])

        for side in range(2):
            weight_copy(side).start()
        row = 0
        for ref, rows in zip(dq_before, before):
            dq_ref[row:row + rows, :] = ref[...]
            row += rows
        dq_ref = dq_ref.at[held:]
    else:
        dq_ref, s_ref = refs
    for index, ref in enumerate(kv_refs):
        ref[...] = jnp.zeros_like(ref) if first else prev_refs[index][...]
    slice_parts = [
        (0, SL, pl.multiple_of(CTX + parity * SL, SL)),
        (SL, REACH, pl.multiple_of(CTX + SL - parity * REACH, REACH)),
    ]

    def block(index, carry):
        def rows_of(ref):
            parts = []
            for j in range(heads):
                lanes = pl.ds(pl.multiple_of((index * heads + j) * HD, HD), HD)
                part = ref[..., lanes]
                if part.size != tokens * HD:
                    part = part.astype(jnp.float32)[:, grad_start:grad_start + tokens // head_count]
                parts.append(part.reshape(tokens, HD).astype(jnp.bfloat16))
            return parts[0] if heads == 1 else jnp.concatenate(parts, axis=0)

        q_rows, g_rows = rows_of(q_ref), rows_of(g_ref)
        delta = jnp.sum(
            g_rows.astype(jnp.float32) * rows_of(o_ref).astype(jnp.float32), axis=1, keepdims=True
        )
        running = None
        for kb in range(cache_blocks):
            keys = slice(kb * KEY_BLOCK, (kb + 1) * KEY_BLOCK)
            scores = dot(q_rows, pair_ref[0, keys, :], NT)
            if (kb + 1) * KEY_BLOCK > CTX // 2:
                scores = scores + bias_c_ref[:, keys]
            s_ref[:, keys] = scores
            top = fold(jnp.maximum, lane_tiles(scores))
            running = top if running is None else jnp.maximum(running, top)
        bias = bias_s_ref[...].reshape(tokens, bias_s_ref.shape[-1])
        bias = bias if heads == 1 else jnp.concatenate([bias] * heads, axis=0)
        for lane, count, row in slice_parts:
            scores = dot(q_rows, pair_ref[0, pl.ds(row, count), :], NT) + bias[:, lane:lane + count]
            s_ref[:, CTX + lane:CTX + lane + count] = scores
            running = jnp.maximum(running, fold(jnp.maximum, lane_tiles(scores)))
        shift = jnp.max(running, axis=1, keepdims=True) * log2_factor

        total = None
        query_grad = None
        for kb in range(cache_blocks):
            keys = slice(kb * KEY_BLOCK, (kb + 1) * KEY_BLOCK)
            probs = jnp.exp2(s_ref[:, keys] * log2_factor - shift)
            part = fold(jnp.add, lane_tiles(probs))
            total = part if total is None else total + part
            prob_grad = dot(g_rows, pair_ref[1, keys, :], NT)
            score_grad = (probs * (prob_grad - delta)).astype(jnp.bfloat16)
            term = dot(score_grad, pair_ref[0, keys, :], NN)
            query_grad = term if query_grad is None else query_grad + term
        probs = jnp.exp2(s_ref[:, CTX:] * log2_factor - shift)
        total = total + fold(jnp.add, lane_tiles(probs))
        scale = 1.0 / jnp.sum(total, axis=1, keepdims=True)
        probs = probs * scale
        query_grad = query_grad * (scale * factor)
        for part, (lane, count, row) in enumerate(slice_parts):
            rows = pl.ds(row, count)
            part_probs = probs[:, lane:lane + count]
            prob_grad = dot(g_rows, pair_ref[1, rows, :], NT)
            score_grad = (part_probs * (prob_grad - delta) * factor).astype(jnp.bfloat16)
            query_grad = query_grad + dot(score_grad, pair_ref[0, rows, :], NN)
            kv_refs[part][:HD, :] += dot(q_rows, score_grad, TN)
            kv_refs[part][HD:, :] += dot(g_rows, part_probs.astype(jnp.bfloat16), TN)
        query_grad = query_grad.astype(jnp.bfloat16)
        for j in range(heads):
            dq_ref[:, pl.ds(pl.multiple_of((index * heads + j) * HD, HD), HD)] = query_grad[
                j * tokens:(j + 1) * tokens
            ]
        return carry

    lax.fori_loop(0, blocks, block, 0)
    if not flush:
        return

    all_rows = refs[1]
    spans, row, place = [], 0, 0
    for rows in (*before, tokens):
        spans.append((row, place, rows // head_count))
        row, place = row + rows, place + rows // head_count
    for side in range(2):
        weight_copy(side).wait()
        column = parity if side == 0 else 1 - parity

        def project(index, carry):
            source = pl.ds(pl.multiple_of(index * tile, tile), tile)
            result = dot(all_rows[...], weights[side, :, source], NN)
            for row, place, count in spans:
                for group in range(head_count):
                    start = row + group * count
                    groups[group, place:place + count] = result[start:start + count]
            lanes = pl.ds(pl.multiple_of(column * half + index * tile, tile), tile)
            for d, out in enumerate(outs):
                out[:, lanes] = groups[head ^ d].astype(jnp.bfloat16)
            return carry

        lax.fori_loop(0, half // tile, project, 0)


def whole_block(array):
    return pl.BlockSpec(array.shape, lambda step: (0,) * array.ndim)


def token_block(array, start, count, head_count, tile):
    width = array.shape[1]
    grouped = array.reshape(head_count, array.shape[0] // head_count, width)
    rows = max(count, tile)
    block = start // rows
    return (
        grouped,
        pl.BlockSpec((head_count, rows, width), lambda step: (0, block, 0)),
        start - block * rows,
    )


def attention(
    stash, grads, pair, bias_c, biases, prev, before, weights, head_count, vmem_limit
):
    tokens, width = stash[0].shape[-2:]
    local_heads = width // HD
    heads = min(local_heads, max(1, ROW_BLOCK // tokens))
    keys = CTX + SL + REACH
    flush = weights is not None
    operands = [(array, whole_block(array)) for array in stash]
    operands += [grads[:2]] + [(array, whole_block(array)) for array in (pair, bias_c)]
    operands += [biases[:2]]
    operands += [(array, whole_block(array)) for array in (*prev, *before)]
    results = [jax.ShapeDtypeStruct((2 * HD, count), jnp.float32) for count in (SL, REACH)]
    scratch = [pltpu.VMEM((heads * tokens, keys), jnp.float32)]
    cost = 3 * tokens * local_heads * keys * HD
    if flush:
        half = weights[0].shape[1]
        tile = min(half, FEATURE_TILE)
        rows = tokens + sum(array.shape[0] for array in before)
        count = rows // head_count
        operands += [(array, pl.BlockSpec(memory_space=pl.ANY)) for array in weights]
        results += [
            jax.ShapeDtypeStruct((count, 2 * half), jnp.bfloat16) for _ in range(head_count)
        ]
        scratch += [
            pltpu.VMEM((rows, width), jnp.bfloat16),
            pltpu.VMEM((2, width, half), jnp.bfloat16),
            pltpu.VMEM((head_count, count, tile), jnp.float32),
            pltpu.SemaphoreType.DMA((2,)),
        ]
        cost += 2 * rows * width * half
    else:
        results += [jax.ShapeDtypeStruct((tokens, width), jnp.bfloat16)]
    outs = pl.pallas_call(
        functools.partial(
            attention_kernel,
            tokens=tokens,
            local_heads=local_heads,
            head_count=head_count,
            paired=len(stash) == 1,
            first=not prev,
            before=tuple(array.shape[0] for array in before),
            flush=flush,
            grad_start=grads[2],
        ),
        out_shape=results,
        grid=(1,),
        in_specs=[spec for _, spec in operands],
        out_specs=[whole_block(result) for result in results],
        scratch_shapes=scratch,
        compiler_params=pltpu.CompilerParams(vmem_limit_bytes=vmem_limit),
        cost_estimate=pl.CostEstimate(
            flops=8 * cost,
            bytes_accessed=4 * tokens * width * 2 + keys * HD * 4,
            transcendentals=tokens * local_heads * keys,
        ),
        name="attention",
    )(*[array for array, _ in operands])
    return outs[:2], outs[2:]


def split_kernel(*refs, sharers):
    head = lax.axis_index("head")
    sources, outs = refs[:2], refs[2:]
    for d, out in enumerate(outs):
        lanes = pl.ds(pl.multiple_of((head ^ d) // sharers * HD, HD), HD)
        for index, source in enumerate(sources):
            out[index] = source[:, lanes]


def split_heads(arrays, head_count):
    rows = arrays[0].shape[0]
    results = [jax.ShapeDtypeStruct((2, rows, HD), arrays[0].dtype) for _ in range(head_count)]
    return pl.pallas_call(
        functools.partial(split_kernel, sharers=head_count // KVH),
        out_shape=results,
        grid=(1,),
        in_specs=[whole_block(array) for array in arrays],
        out_specs=[whole_block(result) for result in results],
        compiler_params=pltpu.CompilerParams(vmem_limit_bytes=VMEM_LIMIT),
        name="split",
    )(*arrays)


def arrange_kernel(*refs):
    pieces, out_ref = refs[:-1], refs[-1]
    parity, head = lax.axis_index("section") % 2, lax.axis_index("head")
    head_count = len(pieces) // 2
    rows = pieces[0].shape[1]
    for index, piece in enumerate(pieces):
        place = parity if index < head_count else 1 - parity
        start = (place * head_count + (head ^ index % head_count)) * rows
        out_ref[:, pl.ds(pl.multiple_of(start, 16), rows)] = piece[...]


def arrange(pieces):
    rows = pieces[0].shape[1]
    result = jax.ShapeDtypeStruct((2, len(pieces) * rows, HD), pieces[0].dtype)
    return pl.pallas_call(
        arrange_kernel,
        out_shape=result,
        grid=(1,),
        in_specs=[whole_block(piece) for piece in pieces],
        out_specs=whole_block(result),
        compiler_params=pltpu.CompilerParams(vmem_limit_bytes=VMEM_LIMIT),
        name="arrange",
    )(*pieces)


def pack_kernel(q_ref, o_ref, *outs, plan, group_tokens, head_count):
    for out, (start, count) in zip(outs, plan):
        for group in range(head_count):
            rows = slice(group * group_tokens + start, group * group_tokens + start + count)
            out[0, group * count:(group + 1) * count] = q_ref[rows]
            out[1, group * count:(group + 1) * count] = o_ref[rows]


def pack(q, o, plan, group_tokens, head_count):
    tokens, width = q.shape
    lanes = min(width, 512)
    return pl.pallas_call(
        functools.partial(
            pack_kernel, plan=plan, group_tokens=group_tokens, head_count=head_count
        ),
        out_shape=[
            jax.ShapeDtypeStruct((2, head_count * count, width), q.dtype) for _, count in plan
        ],
        grid=(width // lanes,),
        in_specs=[pl.BlockSpec((tokens, lanes), lambda step: (0, step))] * 2,
        out_specs=[
            pl.BlockSpec((2, head_count * count, lanes), lambda step: (0, 0, step))
            for _, count in plan
        ],
        name="pack",
    )(q, o)


def transpose_kernel(in_ref, out_ref):
    out_ref[...] = in_ref[...].T


def transposed(array):
    rows, columns = array.shape
    tile = math.gcd(rows, 512)
    return pl.pallas_call(
        transpose_kernel,
        out_shape=jax.ShapeDtypeStruct((columns, rows), array.dtype),
        grid=(rows // tile,),
        in_specs=[pl.BlockSpec((tile, columns), lambda step: (step, 0))],
        out_specs=pl.BlockSpec((columns, tile), lambda step: (0, step)),
        compiler_params=pltpu.CompilerParams(vmem_limit_bytes=VMEM_LIMIT),
        cost_estimate=pl.CostEstimate(
            flops=rows * columns, bytes_accessed=4 * rows * columns, transcendentals=0
        ),
        name="transposed",
    )(array)


def share_kernel(own_ref, recv_ref, *refs):
    outs, total_ref = refs[:-1], refs[-1]
    head = lax.axis_index("head")
    count = outs[0].shape[0]
    parity = lax.axis_index("section") % 2
    lanes = pl.ds(pl.multiple_of((1 - parity) * (SL - REACH), REACH), REACH)
    total_ref[...] = own_ref[...]
    total_ref[:, lanes] += recv_ref[...]
    total = total_ref[...].T
    head_count = len(outs)
    for d, out in enumerate(outs):
        for group in range(head_count):

            @pl.when((head ^ d) == group)
            def _():
                out[...] = total[group * count:(group + 1) * count].astype(out.dtype)


def share_kv(own, recv, head_count, dtype):
    width, tokens = own.shape
    count = tokens // head_count
    results = [jax.ShapeDtypeStruct((count, width), dtype) for _ in range(head_count)]
    return pl.pallas_call(
        share_kernel,
        out_shape=results,
        grid=(1,),
        in_specs=[whole_block(own), whole_block(recv)],
        out_specs=[whole_block(result) for result in results],
        scratch_shapes=[pltpu.VMEM(own.shape, jnp.float32)],
        compiler_params=pltpu.CompilerParams(vmem_limit_bytes=4*2**20),
        cost_estimate=pl.CostEstimate(
            flops=tokens * width, bytes_accessed=tokens * width * 10, transcendentals=0
        ),
        name="share",
    )(own, recv)


def finish_kernel(*refs, plan, head_count, spent):
    shares = len(plan) * head_count
    inputs = 3 + head_count + shares
    sources, refs = refs[:inputs], refs[inputs + spent:]
    weight_sources, refs = refs[:2 * head_count], refs[2 * head_count:]
    out_ref, refs = refs[0], refs[1:]
    locals_, refs = refs[:inputs], refs[inputs:]
    gathered, total_ref, fetched, input_sems, fetch_sems = refs
    distant = range(2, head_count + 1)
    parity, head = lax.axis_index("section") % 2, lax.axis_index("head")
    sharers = head_count // KVH
    width, half = weight_sources[0].shape
    step = min(width, HD)

    def input_copy(index):
        return pltpu.make_async_copy(sources[index], locals_[index], input_sems.at[index])

    def fetch(index):
        slot = index - distant.start
        return pltpu.make_async_copy(weight_sources[index], fetched.at[slot], fetch_sems.at[slot])

    for index in range(3, 3 + head_count):
        input_copy(index).start()
    for index in distant:
        fetch(index).start()
    for index in [*range(3), *range(3 + head_count, inputs)]:
        input_copy(index).start()
    gain_ref, x_ref, res_ref = locals_[:3]
    kv_pieces, pieces = locals_[3:3 + head_count], locals_[3 + head_count:]
    for index in range(3, 3 + head_count):
        input_copy(index).wait()
    if sharers > 1:
        gathered[...] = jnp.zeros_like(gathered)
    for d, piece in enumerate(kv_pieces):
        group = (head ^ d) // sharers
        for part in range(2):
            column = group * HD + part * KVH * HD
            for lane in range(0, HD, step):
                place = (column + lane) // width
                lanes = pl.ds(pl.multiple_of((column + lane) % width, step), step)
                if step == width:
                    lanes = slice(0, width)
                value = piece[:, part * HD + lane:part * HD + lane + step].astype(jnp.float32)
                if sharers > 1:
                    value = gathered[place, :, lanes] + value
                gathered[place, :, lanes] = value
    for side in range(2):
        place = parity if side == 0 else 1 - parity
        lanes = pl.ds(pl.multiple_of(place * half, half), half)
        order = [d for d in range(head_count) if side * head_count + d not in distant]
        order += [d for d in range(head_count) if side * head_count + d in distant]
        terms = []
        for d in order:
            index = side * head_count + d
            left = gathered[head ^ d].astype(jnp.bfloat16)
            if index in distant:
                fetch(index).wait()
                terms.append(dot(left, fetched[index - distant.start], NN))
            else:
                terms.append(dot(left, weight_sources[index][...], NN))
        total_ref[:, lanes] = fold(jnp.add, terms)
    for index in [*range(3), *range(3 + head_count, inputs)]:
        input_copy(index).wait()
    x = x_ref[...].astype(jnp.float32)
    inverse = lax.rsqrt(jnp.mean(x * x, axis=1, keepdims=True) + epsilon)
    for c, (start, count) in enumerate(plan):
        rows = slice(start, start + count)
        parts = [pieces[c * head_count + d][...].astype(jnp.float32) for d in range(head_count)]
        total = total_ref[rows, :] + fold(jnp.add, parts)
        total_ref[rows, :] = gain_ref[...].astype(jnp.float32) * total
    mean = jnp.mean(total_ref[...] * x_ref[...].astype(jnp.float32), axis=1, keepdims=True)
    mean = inverse * inverse * inverse * mean
    out_ref[...] = (
        res_ref[...].astype(jnp.float32)
        + inverse * total_ref[...]
        - x_ref[...].astype(jnp.float32) * mean
    ).astype(out_ref.dtype)


def finish(gain, x, residual, kv_pieces, pieces, spent, weights, plan):
    head_count = len(kv_pieces)
    width, half = weights[0].shape
    rows = x.shape[0]
    local = [gain, x, residual, *kv_pieces, *pieces]
    remote = [*spent, *weights]
    early = [pltpu.HBM] * (len(pieces) - head_count + 1)
    late = [pl.ANY] * (head_count - 1)
    spaces = [pltpu.HBM] * 3 + [pl.ANY] * head_count + early + late
    return pl.pallas_call(
        functools.partial(
            finish_kernel, plan=plan, head_count=head_count, spent=len(spent)
        ),
        out_shape=jax.ShapeDtypeStruct(x.shape, jnp.bfloat16),
        in_specs=[pl.BlockSpec(memory_space=space) for space in spaces]
        + [pl.BlockSpec(memory_space=pltpu.HBM) for _ in spent]
        + [
            pl.BlockSpec(memory_space=pltpu.HBM if 2 <= index <= head_count else pltpu.VMEM)
            for index in range(len(weights))
        ],
        out_specs=pl.BlockSpec(memory_space=pltpu.VMEM),
        scratch_shapes=[pltpu.VMEM(array.shape, array.dtype) for array in local]
        + [
            pltpu.VMEM((head_count, rows, width), jnp.float32),
            pltpu.VMEM((rows, 2 * half), jnp.float32),
            pltpu.VMEM((head_count - 1, width, half), jnp.bfloat16),
            pltpu.SemaphoreType.DMA((len(local),)),
            pltpu.SemaphoreType.DMA((head_count - 1,)),
        ],
        compiler_params=pltpu.CompilerParams(vmem_limit_bytes=24*2**20),
        cost_estimate=pl.CostEstimate(
            flops=512 * half * width * head_count,
            bytes_accessed=4 * half * width * head_count,
            transcendentals=0,
        ),
        name="finish",
    )(*local, *remote)


def body(
    out_grad,
    held_query,
    held_output,
    key_cache,
    value_cache,
    segment_ids,
    image_flags,
    cache_length,
    query_weight,
    kv_weight,
    norm_gain,
    layer_input,
    residual_grad,
):
    head_count = lax.axis_size("head")
    section_count = lax.axis_size("section")
    parity = lax.axis_index("section") % 2
    is_first = parity == 0
    sharers = head_count // KVH
    group_tokens = SL // head_count
    plan = chunk_plan(group_tokens)

    def rows_of_chunk(array, start, count):
        grouped = array.reshape(head_count, group_tokens, array.shape[1])
        return grouped[:, start:start + count].reshape(head_count * count, array.shape[1])

    def swap_cores(value):
        return lax.ppermute(value, "section", xor_pairs("section", 1))

    def ordered(own_value, other_value, axis):
        return jnp.where(
            is_first,
            jnp.concatenate([own_value, other_value], axis),
            jnp.concatenate([other_value, own_value], axis),
        )

    mirror = xor_pairs("section", section_count - 2)
    inward = inward_pairs(section_count)
    first_query = rows_of_chunk(held_query, *plan[0])
    first_query, held_output = lax.optimization_barrier((first_query, held_output))
    first_output = rows_of_chunk(held_output, *plan[0])
    first = [first_query, first_output]
    first_output, held_query, held_output = lax.optimization_barrier(
        (first_output, held_query, held_output)
    )
    buffers = pack(held_query, held_output, plan[1:], group_tokens, head_count)
    buffers, (key_cache, value_cache, kv_weight, query_weight) = lax.optimization_barrier(
        (buffers, (key_cache, value_cache, kv_weight, query_weight))
    )
    stash, spent = [], []
    for c, group in enumerate([first] + [[buffer] for buffer in buffers]):
        stash.append([])
        for buffer in group:
            stash[-1].append(lax.ppermute(buffer, "section", mirror))
        if inward and c in (0, 1):
            spent.append(lax.ppermute(group[0] if c else held_query, "section", inward))

    other_segments = swap_cores(segment_ids)
    other_flags = swap_cores(image_flags)
    other_gain = swap_cores(norm_gain)
    gain = ordered(norm_gain, other_gain, 0)[None, :]

    split = split_heads((key_cache, value_cache), head_count)
    split, (query_weight, kv_weight) = lax.optimization_barrier((split, (query_weight, kv_weight)))
    key_pieces = [split[0]]
    for d in range(1, head_count):
        key_pieces.append(lax.ppermute(split[d], "head", xor_pairs("head", d)))
    for d in range(head_count):
        key_pieces.append(swap_cores(key_pieces[d]))
    pair = arrange(key_pieces)

    positions = jnp.arange(SL, dtype=jnp.int32)
    own_position = parity * SL + positions

    def with_reach(own_values, other_values):
        reach = lax.dynamic_slice_in_dim(other_values, parity * (SL - REACH), REACH)
        return jnp.concatenate([own_values, reach])

    key_position = with_reach(own_position, (1 - parity) * SL + positions)
    key_segments = with_reach(segment_ids, other_segments)
    key_flags = with_reach(image_flags, other_flags)
    visible = (segment_ids[:, None] == key_segments[None, :]) & (
        (key_position[None, :] <= own_position[:, None])
        | ((image_flags[:, None] == 1) & (key_flags[None, :] == 1))
    )
    bias_s = jnp.where(visible, 0.0, far_negative).astype(jnp.float32)
    bias_c = jnp.where(
        jnp.arange(CTX, dtype=jnp.int32)[None, :] < cache_length[0], 0.0, far_negative
    ).astype(jnp.float32)

    query_weight = transposed(query_weight)
    other_weight = swap_cores(query_weight)
    kv_columns = [kv_weight.T]
    for d in range(1, head_count):
        kv_columns.append(lax.ppermute(kv_columns[0], "head", xor_pairs("head", d)))
    for d in range(head_count):
        kv_columns.append(swap_cores(kv_columns[d]))
    gain, bias_c = lax.optimization_barrier((gain, bias_c))

    kv_grad, pieces, spans, before, first_row = (), [], [], [], 0
    flushes = flush_points(plan)
    for c, (start, count) in enumerate(plan):
        kv_grad, parts = attention(
            stash[c],
            token_block(out_grad, start, count, head_count, 16),
            pair,
            bias_c,
            token_block(bias_s, start, count, head_count, 8),
            kv_grad,
            before,
            (query_weight, other_weight) if c in flushes else None,
            head_count,
            VMEM_LIMIT if c + 1 < len(plan) else LAST_VMEM_LIMIT,
        )
        if c not in flushes:
            before = before + list(parts)
            continue
        for d, part in enumerate(parts):
            pieces.append(lax.ppermute(part, "head", xor_pairs("head", d)) if d else part)
        spans.append((first_row, start + count - first_row))
        first_row, before = start + count, []
    received = swap_cores(kv_grad[1])
    share_dtype = jnp.bfloat16 if sharers == 1 else jnp.float32
    shares = list(share_kv(kv_grad[0], received, head_count, share_dtype))
    for d in range(1, head_count):
        shares[d] = lax.ppermute(shares[d], "head", xor_pairs("head", d))
    return finish(
        gain, layer_input, residual_grad, shares, pieces, spent, kv_columns, spans
    )


def solution(mesh):
    return jax.shard_map(
        body,
        mesh=mesh,
        in_specs=(
            P("section", "head"),
            P("section", "head"),
            P("section", "head"),
            P(("section", "head"), None),
            P(("section", "head"), None),
            P("section"),
            P("section"),
            P("section"),
            P("section", "head"),
            P("section", "head"),
            P("section"),
            P(("section", "head"), None),
            P(("section", "head"), None),
        ),
        out_specs=P(("section", "head"), None),
        check_vma=False,
    )
```
